32 devices in a mesh: row: 4 (over x, core), col: 8 (over z, y).
Axes of the slice: x: 2, y: 2, z: 4, core: 2. Of those that a mesh axis runs over, the one named last changes fastest.
Arguments:
- coupling: bfloat16 [32, 4096, 1024], P(('row', 'col')), may hold values from -0.09375 to 0.09375
- modes: bfloat16 [32, 200, 4096], P(('row', 'col')), may hold values from -6 to 6
- flexibility: float32 [32, 200], P(('row', 'col')), may hold values from 0.002 to 0.02
- widths: int32 [32], P(('row', 'col')), may hold values from 512 to 1024
- segments: int32 [32, 8], replicated, may hold values from 0 to 95, as said below
Outputs:
- interface: float32 [12288, 12288], P('row', 'col')
The draws below stay inside these ranges and needn't reach their ends.
Inputs may be any that keep to these rules, and one draw needn't show every extreme that they name: `segments`: the 8 segment numbers of a substructure are distinct, and modulo 16 they are 8 cyclically consecutive residues. `widths`: columns at and beyond a substructure's width are padding.
All inputs are finite; a program needn't handle non-finite values.
Results may differ from the reference program's by a relative error of at most 0.0003.
Values sent between devices are 32-bit elements; how exact they have to be, the bound alone decides.
No kernel may reach another device: no remote copies, remote signals or barrier semaphores. Data moves between devices by JAX's collectives and lax.ppermute only.
A program may use at most 192 MiB of HBM per device.

```python
import math
import jax
import jax.numpy as jnp
from jax import lax

NI = 4096
NB = 1024
MODES = 200
TILE = 128
NG = 12288
RESIDUE_GROUPS = 16
SUBSTRUCT_TOTAL = 32
SEGMENTS_PER_SUB = 8
SEGMENT_TOTAL = 96
N_ROW = 4
N_COL = 8


def draw_segments(key, part):
    first, second_member = jax.random.split(jax.random.fold_in(key, 7))
    start_shift = jax.random.randint(first, (SUBSTRUCT_TOTAL, 1), 0, RESIDUE_GROUPS)
    tree_level = jax.random.randint(second_member, (SUBSTRUCT_TOTAL, SEGMENTS_PER_SUB), 0, SEGMENT_TOTAL // RESIDUE_GROUPS)
    residue_class = (jnp.arange(SEGMENTS_PER_SUB, dtype=jnp.int32)[None, :] + start_shift) % RESIDUE_GROUPS
    return (residue_class + RESIDUE_GROUPS * tree_level).astype(jnp.int32)


def touch_ends(result, rng, low, top_value):
    dims = result.shape
    spot = [jax.random.randint(jax.random.fold_in(rng, axis), (), 0, dims[axis]) for axis in range(len(dims))]
    result = result.at[tuple(spot)].set(low)
    longest = dims.index(max(dims))
    spot[longest] = (spot[longest] + 1) % dims[longest]
    return result.at[tuple(spot)].set(top_value)


def shard_levels(own_key, dims, cuts, least, top_value):
    def one(dim, parts):
        draws = jax.random.uniform(jax.random.fold_in(jax.random.fold_in(own_key, 6), dim), (parts,), jnp.float32, least / len(cuts), top_value / len(cuts))
        return jnp.repeat(jnp.exp(draws), dims[dim] // parts).reshape((-1,) + (1,) * (len(dims) - dim - 1))

    factor_of = one(*cuts[0])
    for cut in cuts[1:]:
        factor_of = factor_of * one(*cut)
    return factor_of


def noise(key, dims, scale, most, cuts=(), kind=jnp.bfloat16):
    array = jax.random.normal(key, dims, jnp.float32) * scale
    if len(cuts) > 0:
        array = shard_levels(key, dims, cuts, -0.22, 0.18) * array
    return jnp.clip(array, min=-most, max=most).astype(kind)


def setup_inputs(seed: int = 0) -> dict:
    seeds = jax.random.split(jax.random.key(seed), 6)
    coupling = noise(seeds[0], (SUBSTRUCT_TOTAL, NI, NB), NI ** -0.5, 0.09375, ((0, 32),))
    modes = noise(seeds[1], (SUBSTRUCT_TOTAL, MODES, NI), 1.0, 6.0, ((0, 32),))
    flexibility = jnp.clip(jnp.exp(math.log(0.02) - 2.30258502 * jax.random.uniform(seeds[2], (SUBSTRUCT_TOTAL, MODES), jnp.float32) ** shard_levels(seeds[2], (SUBSTRUCT_TOTAL, MODES), ((0, 32),), -0.2, 0.2)), 0.002, 0.02)
    widths = touch_ends(jax.random.randint(seeds[3], (SUBSTRUCT_TOTAL,), NB // 2, NB + 1), jax.random.fold_in(seeds[3], 1), NB // 2, NB).astype(jnp.int32)
    segments = draw_segments(jax.random.fold_in(seeds[5], 71), 0)
    return {"coupling": coupling, "modes": modes, "flexibility": flexibility, "widths": widths, "segments": segments}


def substructure_block(factor, modal_rows, weights, width):
    padded = factor.shape[1]
    columns = lax.broadcasted_iota(jnp.int32, (1, padded), 1)
    masked = jnp.where(columns < width, factor, jnp.zeros((), factor.dtype))
    static = lax.dot_general(masked, masked, (((0,), (0,)), ((), ())), preferred_element_type=jnp.float32)
    projected = jnp.dot(modal_rows, masked, preferred_element_type=jnp.float32)
    modal = lax.dot_general(projected * weights[:, None], projected, (((0,), (0,)), ((), ())), precision=lax.Precision.HIGHEST, preferred_element_type=jnp.float32)
    return static - modal

def reference(coupling, modes, flexibility, widths, segments):
    subs_total = coupling.shape[0]
    seg_count = coupling.shape[2] // TILE
    seg_total = NG // TILE

    def add_one(member, matrix):
        block = substructure_block(coupling[member], modes[member], flexibility[member], widths[member])
        tiles = block.reshape(seg_count, TILE, seg_count, TILE).transpose(0, 2, 1, 3)
        placed = segments[member].astype(jnp.int32)
        return matrix.at[placed[:, None], placed[None, :]].add(tiles)
    start = jnp.zeros((seg_total, seg_total, TILE, TILE), jnp.float32)
    matrix = lax.fori_loop(0, subs_total, add_one, start)
    ordinal = jnp.arange(seg_total)
    diag_tiles = matrix[ordinal, ordinal]
    diag_values = jnp.diagonal(diag_tiles, axis1=1, axis2=2)
    scale = 1.0 / jnp.sqrt(1.0 + jnp.abs(diag_values))
    scaled = matrix * scale[:, None, :, None] * scale[None, :, None, :]
    row_order = jnp.arange(seg_total).reshape(seg_total // N_ROW, N_ROW).T.reshape(-1)
    col_order = jnp.arange(seg_total).reshape(seg_total // N_COL, N_COL).T.reshape(-1)
    ordered = scaled[row_order][:, col_order]
    return ordered.transpose(0, 2, 1, 3).reshape(NG, NG)
```

```python
import functools

import jax
import jax.numpy as jnp
from jax import lax
from jax.experimental import pallas as pl
from jax.experimental.pallas import tpu as pltpu
from jax.sharding import Mesh
from jax.sharding import PartitionSpec as P

TILE = 128
NG = 12288


def substructure_block(factor, modal_rows, weights, width):
    padded = factor.shape[1]
    columns = lax.broadcasted_iota(jnp.int32, (1, padded), 1)
    masked = jnp.where(columns < width, factor, jnp.zeros((), factor.dtype))
    static = lax.dot_general(
        masked, masked, (((0,), (0,)), ((), ())), preferred_element_type=jnp.float32
    )
    projected = jnp.dot(modal_rows, masked, preferred_element_type=jnp.float32)
    modal = lax.dot_general(
        projected * weights[:, None],
        projected,
        (((0,), (0,)), ((), ())),
        precision=lax.Precision.HIGHEST,
        preferred_element_type=jnp.float32,
    )
    return static - modal


def rank_among(residue_class):
    count = residue_class.shape[-1]
    places = lax.broadcasted_iota(jnp.int32, (count, count), 0)
    others = lax.broadcasted_iota(jnp.int32, (count, count), 1)
    same = residue_class[..., :, None] == residue_class[..., None, :]
    return jnp.sum(jnp.where(same & (others < places), 1, 0), axis=-1).astype(jnp.int32)


def plain_body(coupling, modes, flexibility, widths, segments):
    row_count = lax.axis_size("row")
    col_count = lax.axis_size("col")
    device_total = row_count * col_count
    local_subs = coupling.shape[0]
    seg_count = coupling.shape[2] // TILE
    seg_total = NG // TILE
    row_tiles = seg_total // row_count
    col_tiles = seg_total // col_count
    row_cap = -(-seg_count // row_count)
    col_cap = -(-seg_count // col_count)
    member_cap = row_cap * col_cap
    capacity = local_subs * member_cap
    slots_all = device_total * capacity
    my_row = lax.axis_index("row")
    my_col = lax.axis_index("col")
    device_id = my_row * col_count + my_col
    blocks = jnp.stack(
        [
            substructure_block(coupling[0], modes[0], flexibility[0], widths[0]).reshape(
                seg_count, TILE, seg_count, TILE
            )
        ]
    )
    mine = lax.dynamic_slice_in_dim(segments, device_id * local_subs, local_subs, 0)
    own_diag = jnp.stack(
        [
            jnp.diagonal(blocks[:, index, :, index, :], axis1=1, axis2=2)
            for index in range(seg_count)
        ],
        axis=1,
    )
    seg_range = lax.broadcasted_iota(jnp.int32, (1, seg_total), 1)
    seg_hot = jnp.where(mine.reshape(-1)[:, None] == seg_range, 1.0, 0.0).astype(jnp.float32)
    partial_diag = lax.dot_general(
        seg_hot,
        own_diag.reshape(local_subs * seg_count, TILE),
        (((0,), (0,)), ((), ())),
        precision=lax.Precision.HIGHEST,
        preferred_element_type=jnp.float32,
    )
    summed_diag = lax.psum(partial_diag, ("row", "col"))
    row_diag = lax.dynamic_index_in_dim(
        summed_diag.reshape(row_tiles, row_count, TILE), my_row, 1, keepdims=False
    )
    col_diag = lax.dynamic_index_in_dim(
        summed_diag.reshape(col_tiles, col_count, TILE), my_col, 1, keepdims=False
    )
    row_res = mine % row_count
    col_res = mine % col_count
    row_rank = rank_among(row_res)
    col_rank = rank_among(col_res)
    member_ids = lax.broadcasted_iota(jnp.int32, (local_subs, seg_count, seg_count), 0)
    target = (
        (row_res[:, :, None] * col_count + col_res[:, None, :]) * capacity
        + member_ids * member_cap
        + row_rank[:, :, None] * col_cap
        + col_rank[:, None, :]
    )
    flat_target = target.reshape(-1)
    slot_ids = lax.broadcasted_iota(jnp.int32, (slots_all, flat_target.shape[0]), 0)
    matches = flat_target[None, :] == slot_ids
    tile_ids = lax.broadcasted_iota(jnp.int32, matches.shape, 1)
    source = jnp.sum(jnp.where(matches, tile_ids, 0), axis=1)
    filled = jnp.any(matches, axis=1)
    per_member = seg_count * seg_count
    member_src = source // per_member
    row_src = source % per_member // seg_count
    col_src = source % seg_count
    outgoing = blocks[member_src, row_src, :, col_src, :]
    outgoing = jnp.where(filled[:, None, None], outgoing, jnp.zeros((), jnp.float32))
    arriving = lax.all_to_all(outgoing, ("row", "col"), split_axis=0, concat_axis=0, tiled=True)
    every_row = segments % row_count
    every_col = segments % col_count
    every_row_rank = rank_among(every_row)
    every_col_rank = rank_among(every_col)
    subs_total = segments.shape[0]
    sub_ids = lax.broadcasted_iota(jnp.int32, (subs_total, seg_count, seg_count), 0)
    keeping = (every_row[:, :, None] == my_row) & (every_col[:, None, :] == my_col)
    placing = (
        sub_ids // local_subs * capacity
        + sub_ids % local_subs * member_cap
        + every_row_rank[:, :, None] * col_cap
        + every_col_rank[:, None, :]
    )
    local_tile = segments[:, :, None] // row_count * col_tiles + segments[:, None, :] // col_count
    keep_flat = keeping.reshape(-1)
    place_flat = placing.reshape(-1)
    tile_flat = local_tile.reshape(-1)
    tile_range = lax.broadcasted_iota(jnp.int32, (1, row_tiles * col_tiles), 1)
    slot_range = lax.broadcasted_iota(jnp.int32, (1, slots_all), 1)
    tile_hot = jnp.where(keep_flat[:, None] & (tile_flat[:, None] == tile_range), 1.0, 0.0).astype(
        jnp.float32
    )
    slot_hot = jnp.where(place_flat[:, None] == slot_range, 1.0, 0.0).astype(jnp.float32)
    routing = lax.dot_general(
        tile_hot,
        slot_hot,
        (((0,), (0,)), ((), ())),
        precision=lax.Precision.HIGHEST,
        preferred_element_type=jnp.float32,
    )
    routing = routing.reshape(row_tiles, col_tiles, slots_all)
    assembled = jnp.einsum(
        "rcp,pxy->rxcy",
        routing,
        arriving,
        precision=lax.Precision.HIGHEST,
        preferred_element_type=jnp.float32,
    )
    row_scale = 1.0 / jnp.sqrt(1.0 + jnp.abs(row_diag))
    col_scale = 1.0 / jnp.sqrt(1.0 + jnp.abs(col_diag))
    scaled = assembled * row_scale[:, :, None, None] * col_scale[None, None, :, :]
    return scaled.reshape(row_tiles * TILE, col_tiles * TILE)


AXES = ("row", "half", "low")
CONTRACT_ROWS = (((0,), (0,)), ((), ()))
VMEM_BYTES = 60 * 1024 * 1024


def place():
    row, half, low = (lax.axis_index(name) for name in AXES)
    low_count = lax.axis_size("low")
    device = (row * lax.axis_size("half") + half) * low_count + low
    return row, half, low, device


def order_segments(segs, order, half, device, seg_count):
    per_half = seg_count // 2
    for index in range(seg_count):
        residue = lax.rem(segs[device, index], seg_count)
        spot = lax.rem(residue, per_half) + jnp.where(residue // per_half == half, per_half, 0)
        order[spot] = index


def fetch(coupling, modes, held, held_modes, sems, order, segments):
    copies = [pltpu.make_async_copy(modes, held_modes, sems.at[segments])]
    copies[0].start()
    for spot in range(segments):
        source = coupling.at[:, pl.ds(pl.multiple_of(order[spot] * TILE, TILE), TILE)]
        copy = pltpu.make_async_copy(source, held.at[:, pl.ds(spot * TILE, TILE)], sems.at[spot])
        copy.start()
        copies.append(copy)
    return copies


def mask_block(held, spot, index, width):
    lanes = lax.broadcasted_iota(jnp.int32, (1, TILE), 1) + index * TILE
    keep = jnp.where(lanes < width, 1.0, 0.0).astype(held.dtype)
    part = pl.ds(spot * TILE, TILE)

    @pl.when((index + 1) * TILE > width)
    def _():
        held[:, part] = held[:, part] * keep


def project(held, held_modes, weights, total, left, right, columns):
    count = held_modes.shape[0]
    padded = left.shape[1]
    spread = jnp.broadcast_to(weights[...], (TILE, padded)).T
    for start in range(0, columns, 2 * TILE):
        part = pl.ds(start, 2 * TILE)
        total[...] = jnp.zeros_like(total)
        total[pl.ds(0, count), :] = jnp.dot(
            held_modes[...], held[:, part], preferred_element_type=jnp.float32
        )
        value = total[...]
        scaled = -value * jnp.concatenate([spread, spread], axis=1)
        high = value.astype(jnp.bfloat16)
        scaled_high = scaled.astype(jnp.bfloat16)
        right[0, :, part] = high
        right[1, :, part] = (value - high.astype(jnp.float32)).astype(jnp.bfloat16)
        left[0, :, part] = scaled_high
        left[1, :, part] = (scaled - scaled_high.astype(jnp.float32)).astype(jnp.bfloat16)


def product(held, left, right, rows, columns):
    rows, columns = pl.ds(*rows), pl.ds(*columns)
    dot = functools.partial(
        lax.dot_general, dimension_numbers=CONTRACT_ROWS, preferred_element_type=jnp.float32
    )
    modal = (
        dot(left[0, :, rows], right[1, :, columns])
        + dot(left[1, :, rows], right[0, :, columns])
        + dot(left[0, :, rows], right[0, :, columns])
    )
    return dot(held[:, rows], held[:, columns]) + modal


def places_in_tile():
    return (
        lax.broadcasted_iota(jnp.int32, (TILE, TILE), 0),
        lax.broadcasted_iota(jnp.int32, (TILE, TILE), 1),
    )


def tile_of(value, row, column):
    return value[row * TILE : (row + 1) * TILE, column * TILE : (column + 1) * TILE]


def upper_tiles(half_tiles):
    return [(a, b) for a in range(half_tiles) for b in range(a + 1, half_tiles)]


def symmetric_tiles(held, left, right, start, half_tiles):
    tiles = {}
    for a in range(0, half_tiles, 2):
        for b in range(a, half_tiles, 2):
            value = product(
                held,
                left,
                right,
                (start + a * TILE, 2 * TILE),
                (start + b * TILE, 2 * TILE),
            )
            for i in range(2):
                for j in range(2):
                    if a + i <= b + j:
                        tiles[a + i, b + j] = tile_of(value, i, j)
    return tiles


def far_kernel(segs, width, weights, coupling, modes, out, order, held, held_modes, total, left, right, sems):
    _, half, _, device = place()
    seg_count = segs.shape[1]
    half_tiles = seg_count // 2
    order_segments(segs, order, half, device, seg_count)
    copies = fetch(coupling, modes, held, held_modes, sems, order, half_tiles)
    for spot, copy in enumerate(copies):
        copy.wait()
        if spot:
            mask_block(held, spot - 1, order[spot - 1], width[0])
    project(held, held_modes, weights, total, left, right, half_tiles * TILE)
    tiles = symmetric_tiles(held, left, right, 0, half_tiles)
    rows, columns = places_in_tile()
    uppers = upper_tiles(half_tiles)
    for spot, pair in enumerate(uppers):
        out[spot] = tiles[pair]
    for a in range(0, half_tiles, 2):
        out[len(uppers) + a // 2] = jnp.where(
            rows <= columns, tiles[a, a], tiles[a + 1, a + 1].T
        )


def near_kernel(segs, width, weights, coupling, modes, mixed, own, diagonals, order, held, held_modes, total, left, right, sems):
    _, half, _, device = place()
    seg_count = segs.shape[1]
    half_tiles = seg_count // 2
    order_segments(segs, order, half, device, seg_count)
    copies = fetch(coupling, modes, held, held_modes, sems, order, seg_count)
    for spot, copy in enumerate(copies):
        copy.wait()
        if spot:
            mask_block(held, spot - 1, order[spot - 1], width[0])
    project(held, held_modes, weights, total, left, right, seg_count * TILE)
    rows, columns = places_in_tile()
    base = half_tiles * TILE
    for a in range(0, half_tiles, 2):
        for b in range(0, half_tiles, 2):
            value = product(held, left, right, (base + a * TILE, 2 * TILE), (b * TILE, 2 * TILE))
            for i in range(2):
                for j in range(2):
                    tile = tile_of(value, i, j)
                    mixed[a + i, 1 - half, b + j] = tile
                    mixed[b + j, half, a + i] = tile.T
    near = symmetric_tiles(held, left, right, base, half_tiles)
    for (a, b), tile in near.items():
        own[a, b] = tile
        if a != b:
            own[b, a] = tile.T
        else:
            diagonals[pl.ds(half * half_tiles + a, 1), :] = jnp.sum(
                jnp.where(rows == columns, tile, 0.0), axis=0, keepdims=True
            )
    for a in range(0, half_tiles, 2):
        value = product(held, left, right, (a * TILE, 2 * TILE), (a * TILE, 2 * TILE))
        for i in range(2):
            diagonals[pl.ds((1 - half) * half_tiles + a + i, 1), :] = jnp.sum(
                jnp.where(rows == columns, tile_of(value, i, i), 0.0), axis=0, keepdims=True
            )


def pack_kernel(own, diagonals, far, far_diagonals, *refs):
    outs, tiles = refs[:-1], refs[-1]
    row, half, low, _ = place()
    half_tiles = own.shape[0]
    rows, columns = places_in_tile()
    uppers = upper_tiles(half_tiles)
    for spot, (a, b) in enumerate(uppers):
        tile = far[spot]
        tiles[a, b] = tile
        tiles[b, a] = tile.T
    for a in range(0, half_tiles, 2):
        tile = far[len(uppers) + a // 2]
        turned = tile.T
        tiles[a, a] = jnp.where(rows <= columns, tile, turned)
        line = far_diagonals[pl.ds(half * half_tiles + a + 1, 1), :]
        second = jnp.where(rows > columns, tile, turned)
        tiles[a + 1, a + 1] = jnp.where(rows == columns, jnp.broadcast_to(line, (TILE, TILE)), second)
    blank = jnp.zeros((1, TILE), jnp.float32)
    for spot, out in enumerate(outs):
        to_row, to_low = row ^ (spot // half_tiles), low ^ (spot % half_tiles)
        out[pl.ds(0, TILE), :] = own[to_row, to_low]
        out[pl.ds(TILE, TILE), :] = tiles[to_row, to_low]
        lines = []
        for source in (diagonals, far_diagonals):
            lines += [
                source[pl.ds(to_row, 1), :],
                source[pl.ds(to_row + half_tiles, 1), :],
                source[pl.ds(half * half_tiles + to_low, 1), :],
                blank,
            ]
        out[pl.ds(2 * TILE, 8), :] = jnp.concatenate(lines, axis=0)


def write_tiles(table, rows_at, tile_at, stage, out, row_scale, col_scale, sem):
    count = stage.shape[0]

    def piece(index):
        row, column = table[rows_at, index], table[rows_at + 1, index]
        return out.at[
            pl.ds(pl.multiple_of(row * TILE, TILE), TILE),
            pl.ds(pl.multiple_of(column * TILE, TILE), TILE),
        ]

    def emit(index, _):
        @pl.when(table[rows_at + 3, index] == 1)
        def _():
            def more(state):
                return state[0] < count

            def add(state):
                spot, value = state
                return table[rows_at + 2, spot], value + tile_at(spot)

            _, value = lax.while_loop(more, add, (table[rows_at + 2, index], tile_at(index)))
            row, column = table[rows_at, index], table[rows_at + 1, index]
            stage[index] = value * row_scale[row] * col_scale[pl.ds(column, 1), :]
            pltpu.make_async_copy(stage.at[index], piece(index), sem).start()

        return 0

    lax.fori_loop(0, count, emit, 0)

    def settle(index, _):
        @pl.when(table[rows_at + 3, index] == 1)
        def _():
            pltpu.make_async_copy(stage.at[index], piece(index), sem).wait()

        return 0

    lax.fori_loop(0, count, settle, 0)


def first_kernel(table, blank, *refs):
    payload_count = len(refs) - 9
    payloads = refs[:payload_count]
    out, row_scale, col_scale, arrived, lines, stage, flat, sems, sem = refs[payload_count:]
    del blank
    copies = []
    for spot, payload in enumerate(payloads):
        copies.append(
            pltpu.make_async_copy(payload.at[pl.ds(0, 2 * TILE), :], arrived.at[spot], sems.at[spot, 0])
        )
        copies.append(
            pltpu.make_async_copy(payload.at[pl.ds(2 * TILE, 8), :], lines.at[spot], sems.at[spot, 1])
        )
    for copy in copies:
        copy.start()
    for copy in copies:
        copy.wait()
    row_count, col_count = row_scale.shape[0], col_scale.shape[0]
    row_ids = lax.broadcasted_iota(jnp.int32, (row_count, TILE), 0)
    col_ids = lax.broadcasted_iota(jnp.int32, (col_count, TILE), 0)
    row_sum = jnp.zeros((row_count, TILE), jnp.float32)
    col_sum = jnp.zeros((col_count, TILE), jnp.float32)
    for spot in range(payload_count):
        for side in range(2):
            index = 2 * spot + side
            for offset in range(2):
                line = lines[spot, pl.ds(4 * side + offset, 1), :]
                row_sum += jnp.where(row_ids == table[8 + offset, index], line, 0.0)
            line = lines[spot, pl.ds(4 * side + 2, 1), :]
            col_sum += jnp.where(col_ids == table[1, index], line, 0.0)
    col_scale[...] = 1.0 / jnp.sqrt(1.0 + jnp.abs(col_sum))
    flat[...] = 1.0 / jnp.sqrt(1.0 + jnp.abs(row_sum))
    for index in range(row_count):
        row_scale[index] = jnp.broadcast_to(flat[pl.ds(index, 1), :], (TILE, TILE)).T

    def tile_at(index):
        return arrived[index // 2, pl.ds(pl.multiple_of(lax.rem(index, 2) * TILE, TILE), TILE), :]

    write_tiles(table, 0, tile_at, stage, out, row_scale, col_scale, sem)


def second_kernel(table, mixed, row_scale, col_scale, filled, out, stage, sem):
    del filled
    write_tiles(table, 4, lambda index: mixed[index], stage, out, row_scale, col_scale, sem)


def chain(rows, columns):
    count = rows.shape[0]
    same = (rows[:, None] == rows[None, :]) & (columns[:, None] == columns[None, :])
    here = lax.broadcasted_iota(jnp.int32, (count, count), 0)
    there = lax.broadcasted_iota(jnp.int32, (count, count), 1)
    after = jnp.min(jnp.where(same & (there > here), there, count), axis=1)
    first = jnp.where(jnp.any(same & (there < here), axis=1), 0, 1)
    return [rows, columns, after, first]


def placements(segments, row, half, low, row_count, low_count):
    col_count = 2 * low_count
    residue = segments % col_count

    def with_residue(wanted):
        return jnp.sum(jnp.where(residue == wanted, segments, 0), axis=1)

    near_rows = with_residue(row + half * low_count) // row_count
    far_rows = with_residue(row + (1 - half) * low_count) // row_count
    columns = with_residue(half * low_count + low) // col_count
    spots = jnp.arange(row_count * low_count)
    source_row, source_low = row ^ (spots // low_count), low ^ (spots % low_count)
    sources = jnp.stack(
        [(source_row * 2 + side) * low_count + source_low for side in (half, 1 - half)], axis=1
    ).reshape(-1)
    lower = jnp.where(half == 0, near_rows, far_rows)
    upper = jnp.where(half == 0, far_rows, near_rows)
    return jnp.stack(
        chain(near_rows[sources], columns[sources])
        + chain(far_rows, columns)
        + [lower[sources], upper[sources]]
    ).astype(jnp.int32)


def whole(memory=pltpu.VMEM):
    return pl.BlockSpec(memory_space=memory)


def fast_body(coupling, modes, flexibility, widths, segments):
    return exchange(coupling, modes, flexibility, widths, segments)


def exchange(coupling, modes, flexibility, widths, segments):
    row_count, low_count = lax.axis_size("row"), lax.axis_size("low")
    row, half, low, _ = place()
    interior, padded = coupling.shape[1:]
    mode_count = modes.shape[1]
    mode_pad = -(-mode_count // 256) * 256
    seg_count = padded // TILE
    half_tiles = seg_count // 2
    seg_total = NG // TILE
    row_tiles, col_tiles = seg_total // row_count, seg_total // (2 * low_count)
    weights = jnp.pad(flexibility, ((0, 0), (0, mode_pad - mode_count)))
    f32, bf16 = jnp.float32, jnp.bfloat16
    params = pltpu.CompilerParams(vmem_limit_bytes=VMEM_BYTES)
    inputs = (segments, widths, weights, coupling[0], modes[0])
    in_specs = [whole(pltpu.SMEM), whole(pltpu.SMEM), whole(), whole(pl.ANY), whole(pl.ANY)]

    def scratch(count):
        return [
            pltpu.SMEM((seg_count,), jnp.int32),
            pltpu.VMEM((interior, count * TILE), bf16),
            pltpu.VMEM((mode_count, interior), bf16),
            pltpu.VMEM((mode_pad, 2 * TILE), f32),
            pltpu.VMEM((2, mode_pad, count * TILE), bf16),
            pltpu.VMEM((2, mode_pad, count * TILE), bf16),
            pltpu.SemaphoreType.DMA((count + 1,)),
        ]

    far_count = len(upper_tiles(half_tiles)) + half_tiles // 2
    far_tiles = pl.pallas_call(
        far_kernel,
        out_shape=jax.ShapeDtypeStruct((far_count, TILE, TILE), f32),
        in_specs=in_specs,
        out_specs=whole(),
        scratch_shapes=scratch(half_tiles),
        compiler_params=params,
        name="far",
        cost_estimate=pl.CostEstimate(flops=4 * 10**9, bytes_accessed=6 * 10**6, transcendentals=0),
    )(*inputs)
    swap = [(0, 1), (1, 0)]
    far_in = lax.ppermute(far_tiles, "half", swap)
    mixed, own, diagonals = pl.pallas_call(
        near_kernel,
        out_shape=[
            jax.ShapeDtypeStruct((row_count, 2, low_count, TILE, TILE), f32),
            jax.ShapeDtypeStruct((half_tiles, half_tiles, TILE, TILE), f32),
            jax.ShapeDtypeStruct((seg_count, TILE), f32),
        ],
        in_specs=in_specs,
        out_specs=[whole()] * 3,
        scratch_shapes=scratch(seg_count),
        compiler_params=params,
        name="near",
        cost_estimate=pl.CostEstimate(flops=8 * 10**9, bytes_accessed=10**7, transcendentals=0),
    )(*inputs)
    far_diagonals = lax.ppermute(diagonals, "half", swap)
    sources = row_count * 2 * low_count
    mixed_in = lax.all_to_all(
        mixed.reshape(sources, TILE, TILE), AXES, split_axis=0, concat_axis=0, tiled=True
    )
    payload = jax.ShapeDtypeStruct((2 * TILE + 8, TILE), f32)
    in_half = row_count * low_count
    payloads = pl.pallas_call(
        pack_kernel,
        out_shape=[payload] * in_half,
        in_specs=[whole()] * 4,
        out_specs=[whole()] * in_half,
        scratch_shapes=[pltpu.VMEM((half_tiles, half_tiles, TILE, TILE), f32)],
        compiler_params=params,
        name="pack",
        cost_estimate=pl.CostEstimate(flops=10**6, bytes_accessed=6 * 10**6, transcendentals=0),
    )(own, diagonals, far_in, far_diagonals)
    arrived = [payloads[0]]
    for spot in range(1, in_half):
        arrived.append(
            lax.ppermute(payloads[spot], ("row", "low"), [(i, i ^ spot) for i in range(in_half)])
        )
    table = placements(segments, row, half, low, row_count, low_count)
    blank = jnp.zeros((row_tiles * TILE, col_tiles * TILE), f32)
    shape = jax.ShapeDtypeStruct(blank.shape, f32)
    filled, row_scale, col_scale = pl.pallas_call(
        first_kernel,
        out_shape=[
            shape,
            jax.ShapeDtypeStruct((row_tiles, TILE, TILE), f32),
            jax.ShapeDtypeStruct((col_tiles, TILE), f32),
        ],
        in_specs=[whole(pltpu.SMEM), whole(pl.ANY)] + [whole(pl.ANY)] * in_half,
        out_specs=[whole(pl.ANY), whole(), whole()],
        scratch_shapes=[
            pltpu.VMEM((in_half, 2 * TILE, TILE), f32),
            pltpu.VMEM((in_half, 8, TILE), f32),
            pltpu.VMEM((2 * in_half, TILE, TILE), f32),
            pltpu.VMEM((row_tiles, TILE), f32),
            pltpu.SemaphoreType.DMA((in_half, 2)),
            pltpu.SemaphoreType.DMA,
        ],
        input_output_aliases={1: 0},
        compiler_params=params,
        name="first",
        cost_estimate=pl.CostEstimate(flops=10**6, bytes_accessed=6 * 10**6, transcendentals=0),
    )(table, blank, *arrived)
    return pl.pallas_call(
        second_kernel,
        out_shape=shape,
        in_specs=[whole(pltpu.SMEM), whole(), whole(), whole(), whole(pl.ANY)],
        out_specs=whole(pl.ANY),
        scratch_shapes=[pltpu.VMEM((sources, TILE, TILE), f32), pltpu.SemaphoreType.DMA],
        input_output_aliases={4: 0},
        compiler_params=params,
        name="second",
        cost_estimate=pl.CostEstimate(flops=10**6, bytes_accessed=6 * 10**6, transcendentals=0),
    )(table, mixed_in, row_scale, col_scale, filled)


def solution(mesh):
    row_count, col_count = mesh.shape["row"], mesh.shape["col"]
    low_count = col_count // 2
    split = Mesh(mesh.devices.reshape(row_count, 2, low_count), AXES)

    def run(coupling, modes, flexibility, widths, segments):
        fits = (
            segments.shape[1] == col_count
            and row_count == low_count
            and row_count & (row_count - 1) == 0
            and segments.shape[0] == row_count * col_count
        )
        axes, used, body = (AXES, split, fast_body) if fits else (("row", "col"), mesh, plain_body)
        in_specs = (P(axes, None, None), P(axes, None, None), P(axes, None), P(axes), P())
        step = jax.shard_map(
            body,
            mesh=used,
            in_specs=in_specs,
            out_specs=P("row", axes[1:]),
            check_vma=False,
        )
        return step(coupling, modes, flexibility, widths, segments)

    return run
```
